32 devices in a mesh: row: 2 (over y), col: 4 (over x, core), rep: 4 (over z).
Axes of the slice: x: 2, y: 2, z: 4, core: 2. Of those that a mesh axis runs over, the one named last changes fastest.
Arguments:
- hidden: bfloat16 [512, 7168], P('rep'), may hold values from -6 to 6
- train_weight: bfloat16 [7168, 16384], P(('rep', 'row'), 'col'), may hold values from -0.0625 to 0.0625
- shard_order: int32 [4, 4, 2], replicated, may hold values from 0 to 1, each once within a row
Outputs:
- served_weight: bfloat16 [7168, 16384], P(None, ('col', 'row'))
- projected: float32 [512, 16384], P('rep', ('col', 'row'))
The draws below stay inside these ranges and needn't reach their ends.
Inputs may be any that keep to these rules, and one draw needn't show every extreme that they name: Each shard_order[c, k] is a permutation of 0 to 1.
All inputs are finite; a program needn't handle non-finite values.
Results may differ from the reference program's by a relative error of at most 0.001.
Values may be sent and summed in bfloat16 or wider, within the bound.
A program may use at most 128 MiB of HBM per device.

```python
import jax
import jax.numpy as jnp

D = 7168
F = 16384
SUB_BLOCKS = 4
SEQS = 512
N_ROW = 2
N_COL = 4


def block_scale(rng, shape, cuts, least, high):
    def one(dim, shards_of):
        heights = jax.random.uniform(jax.random.fold_in(jax.random.fold_in(rng, 6), dim), (shards_of,), jnp.float32, least / len(cuts), high / len(cuts))
        return jnp.repeat(jnp.exp(heights), shape[dim] // shards_of).reshape((-1,) + (1,) * (len(shape) - dim - 1))

    loudness = one(*cuts[0])
    for cut in cuts[1:]:
        loudness = loudness * one(*cut)
    return loudness


def centred(key, extent, width, reach, split=(), dtype=jnp.bfloat16):
    drawn = width * jax.random.normal(key, extent, jnp.float32)
    if split:
        drawn = drawn * block_scale(key, extent, split, -0.22, 0.18)
    return jnp.clip(drawn, -reach, reach).astype(dtype)


def setup_inputs(seed: int = 0) -> dict:
    arg_keys = jax.random.split(jax.random.key(seed), 4)
    hidden = centred(arg_keys[0], (SEQS, D), 1.0, 6.0, ((0, 4),))
    train_weight = centred(arg_keys[1], (D, F), D ** -0.5, 0.0625, ((0, 8), (1, 4)))
    shard_order = jax.vmap(lambda own: jax.random.permutation(own, N_ROW))(jax.random.split(arg_keys[2], N_COL * SUB_BLOCKS)).reshape((N_COL, SUB_BLOCKS, N_ROW)).astype(jnp.int32)
    return dict(hidden=hidden, train_weight=train_weight, shard_order=shard_order)


def reference(hidden, train_weight, shard_order):
    block_cols = F // (N_ROW * N_COL)
    sub_cols = block_cols // SUB_BLOCKS
    blocks = train_weight.reshape(D, N_COL, N_ROW, SUB_BLOCKS, sub_cols)
    order = shard_order.astype(jnp.int32)
    pieces = []
    for index in range(SUB_BLOCKS):
        subset = blocks[:, :, :, index, :]
        picks = jnp.broadcast_to(order[:, index, :][None, :, :, None], subset.shape)
        pieces.append(jnp.take_along_axis(subset, picks, axis=2))
    served = jnp.stack(pieces, axis=3).reshape(D, F)
    projected = jnp.dot(hidden, served, preferred_element_type=jnp.float32)
    return served, projected
```

```python
import functools

import jax
import jax.numpy as jnp
from jax import lax
from jax.experimental import pallas as pl
from jax.experimental.pallas import tpu as pltpu
from jax.sharding import PartitionSpec as P

MESH = pl.DeviceIdType.MESH
LANES = 128
VMEM_LIMIT = 8 * 1024 * 1024


def order_kernel(order_ref, tile_ref, out_ref, sem):
    _, sub_count, row_count = order_ref.shape
    c = lax.axis_index("col")
    piece_cols = out_ref.shape[2]
    sub_cols = piece_cols // sub_count
    copies = []
    for s in range(row_count):
        for k in range(sub_count):
            start = pl.multiple_of(order_ref[c, k, s] * piece_cols + k * sub_cols, LANES)
            copies.append(
                pltpu.make_async_copy(
                    tile_ref.at[:, pl.ds(start, sub_cols)],
                    out_ref.at[s, :, pl.ds(k * sub_cols, sub_cols)],
                    sem.at[s * sub_count + k],
                )
            )
    for copy in copies:
        copy.start()
    for copy in copies:
        copy.wait()


def ordered_pieces(tile, shard_order):
    _, sub_count, row_count = shard_order.shape
    rows_tile, cols_tile = tile.shape
    piece_cols = cols_tile // row_count
    sub_cols = piece_cols // sub_count
    if sub_cols % LANES == 0:
        return pl.pallas_call(
            order_kernel,
            out_shape=pltpu.VMEM((row_count, rows_tile, piece_cols), tile.dtype),
            in_specs=[
                pl.BlockSpec(memory_space=pltpu.SMEM),
                pl.BlockSpec(memory_space=pltpu.HBM),
            ],
            out_specs=pl.BlockSpec(memory_space=pltpu.VMEM),
            scratch_shapes=[pltpu.SemaphoreType.DMA((row_count * sub_count,))],
            compiler_params=pltpu.CompilerParams(vmem_limit_bytes=VMEM_LIMIT),
        )(shard_order, pltpu.with_memory_space_constraint(tile, pltpu.HBM))
    my_order = lax.dynamic_index_in_dim(shard_order, lax.axis_index("col"), 0, keepdims=False)
    blocks = tile.reshape(rows_tile, row_count, sub_count, sub_cols)
    pieces = []
    for s in range(row_count):
        piece = blocks[:, 0]
        for j in range(1, row_count):
            piece = jnp.where((my_order[:, s] == j)[None, :, None], blocks[:, j], piece)
        pieces.append(piece.reshape(rows_tile, piece_cols))
    return jnp.stack(pieces)


def gather_kernel(n_row, n_rep, chunks, own_ref, out_ref, y_send, y_recv, z_recv, up_send, down_send):
    r, c, z = lax.axis_index("row"), lax.axis_index("col"), lax.axis_index("rep")
    rows_tile = own_ref.shape[1]
    rows = rows_tile // chunks
    has_up, has_down = z < n_rep - 1, z > 0
    above = (r, c, jnp.minimum(z + 1, n_rep - 1))
    below = (r, c, jnp.maximum(z - 1, 0))
    per_level = n_row * chunks

    barrier = pltpu.get_barrier_semaphore()
    for t in range(1, n_row):
        pl.semaphore_signal(barrier, inc=1, device_id=(lax.rem(r + t, n_row), c, z), device_id_type=MESH)

    @pl.when(has_up)
    def _():
        pl.semaphore_signal(barrier, inc=1, device_id=above, device_id_type=MESH)

    @pl.when(has_down)
    def _():
        pl.semaphore_signal(barrier, inc=1, device_id=below, device_id_type=MESH)

    pl.semaphore_wait(barrier, n_row - 1 + has_up.astype(jnp.int32) + has_down.astype(jnp.int32))

    def part(ref, block, q):
        if ref is own_ref:
            return ref.at[block, pl.ds(pl.multiple_of(q * rows, 8), rows)]
        return ref.at[pl.ds(pl.multiple_of(block * rows_tile + q * rows, 8), rows)]

    def along_row(t, q, outward):
        peer = lax.rem(r + t, n_row)
        return pltpu.make_async_remote_copy(
            src_ref=part(own_ref, peer, q),
            dst_ref=part(out_ref, z * n_row + r if outward else z * n_row + lax.rem(r - t + n_row, n_row), q),
            send_sem=y_send.at[t * chunks + q],
            recv_sem=y_recv.at[t * chunks + q],
            device_id=(peer, c, z),
            device_id_type=MESH,
        )

    def along_rep(source, block, q, sems, target):
        return pltpu.make_async_remote_copy(
            src_ref=part(*source, q),
            dst_ref=part(out_ref, block, q),
            send_sem=sems.at[block * chunks + q],
            recv_sem=z_recv.at[block * chunks + q],
            device_id=target,
            device_id_type=MESH,
        )

    def forward(source, block, q):
        @pl.when(has_up)
        def _():
            along_rep(source, block, q, up_send, above).start()

        @pl.when(has_down)
        def _():
            along_rep(source, block, q, down_send, below).start()

    mine = z * n_row + r

    @pl.loop(0, chunks)
    def _(q):
        forward((own_ref, r), mine, q)
        for t in range(1, n_row):
            along_row(t, q, True).start()

    step = 16 if rows_tile % 16 == 0 else 8

    @pl.loop(0, rows_tile // step)
    def _(i):
        at = pl.ds(pl.multiple_of(i * step, step), step)
        to = pl.ds(pl.multiple_of(mine * rows_tile + i * step, step), step)
        out_ref[to, :] = own_ref[r, at, :]

    for t in range(1, n_row):

        @pl.loop(0, chunks)
        def _(q):
            along_row(t, q, False).wait_recv()
            block = z * n_row + lax.rem(r - t + n_row, n_row)
            forward((out_ref, block), block, q)

    def arrived(level, i, sems, target, onward):
        t, q = i // chunks, lax.rem(i, chunks)
        block = level * n_row + lax.rem(r - t + n_row, n_row)
        copy = along_rep((out_ref, block), block, q, sems, target)
        copy.wait_recv()

        @pl.when(onward)
        def _():
            copy.start()

    @pl.loop(1, n_rep)
    def _(d):
        @pl.loop(0, per_level)
        def _(i):
            @pl.when(z - d >= 0)
            def _():
                arrived(z - d, i, up_send, above, has_up)

            @pl.when(z + d < n_rep)
            def _():
                arrived(z + d, i, down_send, below, has_down)

    @pl.loop(0, chunks)
    def _(q):
        for t in range(1, n_row):
            along_row(t, q, True).wait_send()

    def drain(first, last, sems, target):
        @pl.loop(first * per_level, last * per_level)
        def _(i):
            block, q = i // chunks, lax.rem(i, chunks)
            along_rep((out_ref, block), block, q, sems, target).wait_send()

    @pl.when(has_up)
    def _():
        drain(0, z + 1, up_send, above)

    @pl.when(has_down)
    def _():
        drain(z, n_rep, down_send, below)


def gathered(own):
    n_row, n_rep = lax.axis_size("row"), lax.axis_size("rep")
    _, rows_tile, piece_cols = own.shape
    chunks = 4 if rows_tile % 64 == 0 else 1
    every = n_rep * n_row * chunks
    dma = pltpu.SemaphoreType.DMA
    return pl.pallas_call(
        functools.partial(gather_kernel, n_row, n_rep, chunks),
        out_shape=pltpu.VMEM((n_rep * n_row * rows_tile, piece_cols), own.dtype),
        in_specs=[pl.BlockSpec(memory_space=pltpu.VMEM)],
        out_specs=pl.BlockSpec(memory_space=pltpu.VMEM),
        scratch_shapes=[
            dma((n_row * chunks,)),
            dma((n_row * chunks,)),
            dma((every,)),
            dma((every,)),
            dma((every,)),
        ],
        compiler_params=pltpu.CompilerParams(
            collective_id=0, has_side_effects=True, vmem_limit_bytes=VMEM_LIMIT
        ),
    )(pltpu.with_memory_space_constraint(own, pltpu.VMEM))


def project_kernel(hidden_ref, landed_ref, served_ref, projected_ref, sem):
    parts = sem.shape[0]
    rows = served_ref.shape[0] // parts
    cols = served_ref.shape[1]
    copies = [
        pltpu.make_async_copy(
            landed_ref.at[pl.ds(i * rows, rows)], served_ref.at[pl.ds(i * rows, rows)], sem.at[i]
        )
        for i in range(parts)
    ]
    for copy in copies:
        copy.start()
    tile = 256 if cols % 256 == 0 else LANES

    @pl.loop(0, cols // tile)
    def _(n):
        at = pl.ds(pl.multiple_of(n * tile, tile), tile)
        projected_ref[:, at] = jnp.dot(
            hidden_ref[...], landed_ref[:, at], preferred_element_type=jnp.float32
        )

    for copy in copies:
        copy.wait()


def projected_and_stored(hidden, landed):
    rows, cols = landed.shape
    return pl.pallas_call(
        project_kernel,
        out_shape=(
            jax.ShapeDtypeStruct(landed.shape, landed.dtype),
            jax.ShapeDtypeStruct((hidden.shape[0], cols), jnp.float32),
        ),
        in_specs=[pl.BlockSpec(memory_space=pltpu.VMEM)] * 2,
        out_specs=(
            pl.BlockSpec(memory_space=pl.ANY),
            pl.BlockSpec(memory_space=pltpu.VMEM),
        ),
        scratch_shapes=[pltpu.SemaphoreType.DMA((8,))],
        compiler_params=pltpu.CompilerParams(vmem_limit_bytes=VMEM_LIMIT),
    )(hidden, pltpu.with_memory_space_constraint(landed, pltpu.VMEM))


def shards(hidden, train_weight, shard_order):
    landed = gathered(ordered_pieces(train_weight, shard_order))
    return projected_and_stored(hidden, landed)


def solution(mesh):
    placed = (P("rep", None), P(("rep", "row"), "col"), P())
    return jax.shard_map(
        shards,
        mesh=mesh,
        in_specs=placed,
        out_specs=(P(None, ("col", "row")), P("rep", ("col", "row"))),
        check_vma=False,
    )
```

```python
import functools

import jax
import jax.numpy as jnp
from jax import lax
from jax.experimental import pallas as pl
from jax.experimental.pallas import tpu as pltpu
from jax.sharding import PartitionSpec as P

MESH = pl.DeviceIdType.MESH
LANES = 128
VMEM_LIMIT = 8 * 1024 * 1024


def order_kernel(order_ref, tile_ref, out_ref, sem):
    _, sub_count, row_count = order_ref.shape
    c = lax.axis_index("col")
    piece_cols = out_ref.shape[2]
    sub_cols = piece_cols // sub_count
    copies = []
    for s in range(row_count):
        for k in range(sub_count):
            start = pl.multiple_of(order_ref[c, k, s] * piece_cols + k * sub_cols, LANES)
            copies.append(
                pltpu.make_async_copy(
                    tile_ref.at[:, pl.ds(start, sub_cols)],
                    out_ref.at[s, :, pl.ds(k * sub_cols, sub_cols)],
                    sem.at[s * sub_count + k],
                )
            )
    for copy in copies:
        copy.start()
    for copy in copies:
        copy.wait()


def ordered_pieces(tile, shard_order):
    _, sub_count, row_count = shard_order.shape
    rows_tile, cols_tile = tile.shape
    piece_cols = cols_tile // row_count
    sub_cols = piece_cols // sub_count
    if sub_cols % LANES == 0:
        return pl.pallas_call(
            order_kernel,
            out_shape=pltpu.VMEM((row_count, rows_tile, piece_cols), tile.dtype),
            in_specs=[
                pl.BlockSpec(memory_space=pltpu.SMEM),
                pl.BlockSpec(memory_space=pltpu.HBM),
            ],
            out_specs=pl.BlockSpec(memory_space=pltpu.VMEM),
            scratch_shapes=[pltpu.SemaphoreType.DMA((row_count * sub_count,))],
            compiler_params=pltpu.CompilerParams(vmem_limit_bytes=VMEM_LIMIT),
        )(shard_order, pltpu.with_memory_space_constraint(tile, pltpu.HBM))
    my_order = lax.dynamic_index_in_dim(shard_order, lax.axis_index("col"), 0, keepdims=False)
    blocks = tile.reshape(rows_tile, row_count, sub_count, sub_cols)
    pieces = []
    for s in range(row_count):
        piece = blocks[:, 0]
        for j in range(1, row_count):
            piece = jnp.where((my_order[:, s] == j)[None, :, None], blocks[:, j], piece)
        pieces.append(piece.reshape(rows_tile, piece_cols))
    return jnp.stack(pieces)


def gather_kernel(n_row, n_rep, chunks, own_ref, hidden_ref, out_ref, projected_ref, y_send, y_recv, z_recv, up_send, down_send):
    r, c, z = lax.axis_index("row"), lax.axis_index("col"), lax.axis_index("rep")
    rows_tile = own_ref.shape[1]
    rows = rows_tile // chunks
    has_up, has_down = z < n_rep - 1, z > 0
    above = (r, c, jnp.minimum(z + 1, n_rep - 1))
    below = (r, c, jnp.maximum(z - 1, 0))
    per_level = n_row * chunks

    barrier = pltpu.get_barrier_semaphore()
    for t in range(1, n_row):
        pl.semaphore_signal(barrier, inc=1, device_id=(lax.rem(r + t, n_row), c, z), device_id_type=MESH)

    @pl.when(has_up)
    def _():
        pl.semaphore_signal(barrier, inc=1, device_id=above, device_id_type=MESH)

    @pl.when(has_down)
    def _():
        pl.semaphore_signal(barrier, inc=1, device_id=below, device_id_type=MESH)

    pl.semaphore_wait(barrier, n_row - 1 + has_up.astype(jnp.int32) + has_down.astype(jnp.int32))

    def part(ref, block, q):
        if ref is own_ref:
            return ref.at[block, pl.ds(pl.multiple_of(q * rows, 8), rows)]
        return ref.at[pl.ds(pl.multiple_of(block * rows_tile + q * rows, 8), rows)]

    def along_row(t, q, outward):
        peer = lax.rem(r + t, n_row)
        return pltpu.make_async_remote_copy(
            src_ref=part(own_ref, peer, q),
            dst_ref=part(out_ref, z * n_row + r if outward else z * n_row + lax.rem(r - t + n_row, n_row), q),
            send_sem=y_send.at[t * chunks + q],
            recv_sem=y_recv.at[t * chunks + q],
            device_id=(peer, c, z),
            device_id_type=MESH,
        )

    def along_rep(source, block, q, sems, target):
        return pltpu.make_async_remote_copy(
            src_ref=part(*source, q),
            dst_ref=part(out_ref, block, q),
            send_sem=sems.at[block * chunks + q],
            recv_sem=z_recv.at[block * chunks + q],
            device_id=target,
            device_id_type=MESH,
        )

    def forward(source, block, q):
        @pl.when(has_up)
        def _():
            along_rep(source, block, q, up_send, above).start()

        @pl.when(has_down)
        def _():
            along_rep(source, block, q, down_send, below).start()

    level_rows = n_row * rows_tile
    by_level = level_rows % LANES == 0
    cols = out_ref.shape[1]
    tile = 256 if cols % 256 == 0 else LANES

    def multiply(first, depth, fresh):
        within = pl.ds(first, depth)

        @pl.loop(0, cols // tile)
        def _(n):
            at = pl.ds(pl.multiple_of(n * tile, tile), tile)
            term = jnp.dot(
                hidden_ref[:, within], out_ref[within, at], preferred_element_type=jnp.float32
            )
            projected_ref[:, at] = term if fresh else projected_ref[:, at] + term

    def add_level(level, fresh=False):
        if by_level:
            multiply(pl.multiple_of(level * level_rows, LANES), level_rows, fresh)

    mine = z * n_row + r

    @pl.loop(0, chunks)
    def _(q):
        forward((own_ref, r), mine, q)
        for t in range(1, n_row):
            along_row(t, q, True).start()

    step = 16 if rows_tile % 16 == 0 else 8

    @pl.loop(0, rows_tile // step)
    def _(i):
        at = pl.ds(pl.multiple_of(i * step, step), step)
        to = pl.ds(pl.multiple_of(mine * rows_tile + i * step, step), step)
        out_ref[to, :] = own_ref[r, at, :]

    for t in range(1, n_row):

        @pl.loop(0, chunks)
        def _(q):
            along_row(t, q, False).wait_recv()
            block = z * n_row + lax.rem(r - t + n_row, n_row)
            forward((out_ref, block), block, q)

    def arrived(level, i, sems, target, onward):
        t, q = i // chunks, lax.rem(i, chunks)
        block = level * n_row + lax.rem(r - t + n_row, n_row)
        copy = along_rep((out_ref, block), block, q, sems, target)
        copy.wait_recv()

        @pl.when(onward)
        def _():
            copy.start()

    add_level(z, True)

    @pl.loop(1, n_rep)
    def _(d):
        @pl.loop(0, per_level)
        def _(i):
            @pl.when(z - d >= 0)
            def _():
                arrived(z - d, i, up_send, above, has_up)

            @pl.when(z + d < n_rep)
            def _():
                arrived(z + d, i, down_send, below, has_down)

        @pl.when(z - d >= 0)
        def _():
            add_level(z - d)

        @pl.when(z + d < n_rep)
        def _():
            add_level(z + d)

    if not by_level:
        multiply(0, out_ref.shape[0], True)

    @pl.loop(0, chunks)
    def _(q):
        for t in range(1, n_row):
            along_row(t, q, True).wait_send()

    def drain(first, last, sems, target):
        @pl.loop(first * per_level, last * per_level)
        def _(i):
            block, q = i // chunks, lax.rem(i, chunks)
            along_rep((out_ref, block), block, q, sems, target).wait_send()

    @pl.when(has_up)
    def _():
        drain(0, z + 1, up_send, above)

    @pl.when(has_down)
    def _():
        drain(z, n_rep, down_send, below)


def gathered(own, hidden):
    n_row, n_rep = lax.axis_size("row"), lax.axis_size("rep")
    _, rows_tile, piece_cols = own.shape
    chunks = 4 if rows_tile % 64 == 0 else 1
    every = n_rep * n_row * chunks
    dma = pltpu.SemaphoreType.DMA
    return pl.pallas_call(
        functools.partial(gather_kernel, n_row, n_rep, chunks),
        out_shape=(
            pltpu.VMEM((n_rep * n_row * rows_tile, piece_cols), own.dtype),
            pltpu.VMEM((hidden.shape[0], piece_cols), jnp.float32),
        ),
        in_specs=[pl.BlockSpec(memory_space=pltpu.VMEM)] * 2,
        out_specs=(pl.BlockSpec(memory_space=pltpu.VMEM),) * 2,
        scratch_shapes=[
            dma((n_row * chunks,)),
            dma((n_row * chunks,)),
            dma((every,)),
            dma((every,)),
            dma((every,)),
        ],
        compiler_params=pltpu.CompilerParams(
            collective_id=0, has_side_effects=True, vmem_limit_bytes=VMEM_LIMIT
        ),
    )(pltpu.with_memory_space_constraint(own, pltpu.VMEM), hidden)


def store_kernel(landed_ref, served_ref, sem):
    parts = sem.shape[0]
    rows = served_ref.shape[0] // parts
    copies = [
        pltpu.make_async_copy(
            landed_ref.at[pl.ds(i * rows, rows)], served_ref.at[pl.ds(i * rows, rows)], sem.at[i]
        )
        for i in range(parts)
    ]
    for copy in copies:
        copy.start()
    for copy in copies:
        copy.wait()


def stored(landed):
    return pl.pallas_call(
        store_kernel,
        out_shape=jax.ShapeDtypeStruct(landed.shape, landed.dtype),
        in_specs=[pl.BlockSpec(memory_space=pl.ANY)],
        out_specs=pl.BlockSpec(memory_space=pl.ANY),
        scratch_shapes=[pltpu.SemaphoreType.DMA((8,))],
        compiler_params=pltpu.CompilerParams(vmem_limit_bytes=1024 * 1024),
    )(landed)


def shards(hidden, train_weight, shard_order):
    landed, projected = gathered(ordered_pieces(train_weight, shard_order), hidden)
    return stored(landed), projected


def solution(mesh):
    placed = (P("rep", None), P(("rep", "row"), "col"), P())
    return jax.shard_map(
        shards,
        mesh=mesh,
        in_specs=placed,
        out_specs=(P(None, ("col", "row")), P("rep", ("col", "row"))),
        check_vma=False,
    )
```
